32 devices in a mesh: groups: 2 (over x), seq: 16 (over z, y, core).
Axes of the slice: x: 2, y: 2, z: 4, core: 2. Of those that a mesh axis runs over, the one named last changes fastest.
Arguments:
- query: bfloat16 [256, 4096], P(('groups', 'seq')), parts along dimension 0, may hold values from -4 to 4
- kv_pages: bfloat16 [1280, 2, 128, 512], P(('groups', 'seq')), parts along dimension 0, may hold values from -512 to 512
- page_table: int32 [256, 128], P('groups'), parts along dimension 0, may hold values from -1 to 639, as said below
- context_len: int32 [256], P('groups'), parts along dimension 0, may hold values from 1 to 16384, as said below
Outputs:
- attended: bfloat16 [256, 4096], P(('groups', 'seq')), parts along dimension 0
The draws below stay inside these ranges and needn't reach their ends.
There are 2 independent parts, one for each index of `groups`. The reference program is written for one: setup_inputs(seed, part) draws one part's arguments, and reference() takes and returns one part's arrays. A program takes and returns all parts, laid end to end along the dimension named above; each array names one. Nothing has to cross between parts.
Inputs may be any that keep to these rules, and one draw needn't show every extreme that they name: `page_table`: entries of request r at slots below ceil(context_len[r] / 128) are page slots, no slot appears twice in the table; all other entries are -1. `context_len`: some request has exactly 16384 tokens.
All inputs are finite; a program needn't handle non-finite values.
Results may differ from the reference program's by a relative error of at most 0.0036.
Values may be sent and summed in bfloat16 or wider, within the bound.
A program may use at most 128 MiB of HBM per device.

```python
import jax
import jax.numpy as jnp
from jax import lax

HQ = 32
KVH = 4
DH = 128
PAGE = 128
PAGES_DEV = 40
MAXPAGES = 128
REQUESTS = 128
PAGES = 640
LIVE = 384


def allocate(key):
    base = jax.random.fold_in(key, 101)
    key_one, key_two, key_three, key_four, key_five = jax.random.split(base, 5)
    shares = jax.random.randint(key_one, (REQUESTS,), 1, 1024)
    counts = 1 + shares * (LIVE - REQUESTS) // jnp.sum(shares)
    counts = jnp.minimum(counts, MAXPAGES)
    chosen = jax.random.randint(key_two, (), 0, REQUESTS)
    rows = jnp.arange(REQUESTS, dtype=jnp.int32)
    counts = jnp.where(rows == chosen, MAXPAGES, counts)
    lengths = (counts - 1) * PAGE + jax.random.randint(key_three, (REQUESTS,), 1, PAGE + 1)
    lengths = jnp.where(rows == chosen, MAXPAGES * PAGE, lengths)
    devices = PAGES // PAGES_DEV
    biases = jax.random.randint(key_four, (devices,), 0, 6144)
    noise = jax.random.randint(key_five, (PAGES,), 0, 4096)
    scores = (noise + jnp.repeat(biases, PAGES_DEV)) * PAGES + jnp.arange(PAGES, dtype=jnp.int32)
    order = jnp.argsort(scores, stable=True).astype(jnp.int32)
    starts = jnp.cumsum(counts) - counts
    slots = jnp.arange(MAXPAGES, dtype=jnp.int32)
    places = jnp.minimum(starts[:, None] + slots[None, :], PAGES - 1)
    table = jnp.where(slots[None, :] < counts[:, None], order[places], -1)
    return (table.astype(jnp.int32), lengths.astype(jnp.int32))


def draw_page_table(key, part):
    return allocate(key)[0]


def draw_context_len(key, part):
    return allocate(key)[1]


def draw_query(key, part):
    base = jax.random.fold_in(key, 202)
    key_two = jax.random.fold_in(base, 1)
    values = jax.random.normal(key_two, (REQUESTS, HQ * DH), jnp.float32)
    return jnp.clip(values, -4.0, 4.0).astype(jnp.bfloat16)


def draw_kv_pages(key, part):
    base = jax.random.fold_in(key, 303)
    key_two = jax.random.fold_in(base, 1)
    values = jnp.clip(jax.random.normal(key_two, (PAGES, 2, PAGE, KVH * DH), jnp.float32), -4.0, 4.0)
    return values.astype(jnp.bfloat16)


def setup_inputs(seed: int = 0, part: int = 0) -> dict:
    key_list = jax.random.split(jax.random.key(seed), 5)
    own_keys = jax.random.split(jax.random.fold_in(key_list[4], part), 5)
    return {
        "query": draw_query(jax.random.fold_in(jax.random.fold_in(key_list[4], part), 71), part),
        "kv_pages": draw_kv_pages(jax.random.fold_in(jax.random.fold_in(key_list[4], part), 71), part),
        "page_table": draw_page_table(jax.random.fold_in(jax.random.fold_in(key_list[4], part), 71), part),
        "context_len": draw_context_len(jax.random.fold_in(jax.random.fold_in(key_list[4], part), 71), part),
    }


def reference(query, kv_pages, page_table, context_len):
    groups = HQ // KVH
    scale = DH ** -0.5

    def single(item):
        row, table_row, length = item
        index = jnp.maximum(table_row, 0).astype(jnp.int32)
        pages = jnp.take(kv_pages, index, axis=0)
        keys = pages[:, 0].reshape(MAXPAGES * PAGE, KVH, DH).astype(jnp.float32)
        values = pages[:, 1].reshape(MAXPAGES * PAGE, KVH, DH).astype(jnp.float32)
        heads = row.reshape(KVH, groups, DH).astype(jnp.float32)
        scores = jnp.einsum("gqd,tgd->gqt", heads, keys, precision=lax.Precision.HIGHEST) * scale
        valid = jnp.arange(MAXPAGES * PAGE, dtype=jnp.int32) < length
        scores = jnp.where(valid[None, None, :], scores, jnp.float32(-1e30))
        peak = jnp.max(scores, axis=2, keepdims=True)
        weights = jnp.where(valid[None, None, :], jnp.exp(scores - peak), jnp.float32(0.0))
        total = jnp.sum(weights, axis=2)
        rounded = lax.optimization_barrier(weights.astype(jnp.bfloat16)).astype(jnp.float32)
        numer = jnp.einsum("gqt,tgd->gqd", rounded, values, precision=lax.Precision.HIGHEST)
        return (numer / total[:, :, None]).reshape(HQ * DH).astype(jnp.bfloat16)

    return lax.map(single, (query, page_table, context_len))
```

```python
import functools

import jax
import jax.numpy as jnp
from jax import lax
from jax.experimental import pallas as pl
from jax.experimental.pallas import tpu as pltpu
from jax.sharding import PartitionSpec as P

HQ = 32
KVH = 4
DH = 128
LOW = -1e30


def kernel(
    n, req_dev, pages_dev, page_len, scale,
    meta, q_ref, kv_ref, o_ref,
    kv, qg, qtmp, bd, pn, pm, pt, snd, rcv, mls, mlr, wts, wtt, acc,
    kv_sem, q_send, f_send, q_recv, a_send, a_recv, m_send, m_recv,
):
    me = lax.axis_index("seq")
    groups = HQ // KVH
    chips = n // 2
    sib = me + 1 - 2 * lax.rem(me, 2)
    per_block = 128 // req_dev
    blocks = n // per_block

    def kv_copy(p):
        return pltpu.make_async_copy(kv_ref.at[p], kv.at[p], kv_sem.at[p])

    @pl.loop(0, pages_dev)
    def _(p):
        kv_copy(p).start()

    barrier = pltpu.get_barrier_semaphore()

    @pl.loop(1, n)
    def _(k):
        pl.semaphore_signal(barrier, inc=1, device_id={"seq": lax.rem(me + k, n)})

    for h in range(HQ):
        qtmp[pl.ds(h, req_dev, stride=HQ), :] = q_ref[:, h * DH:(h + 1) * DH].astype(jnp.float32)
    qg[me] = qtmp[...].astype(jnp.bfloat16).reshape(req_dev, HQ, DH)
    row = lax.broadcasted_iota(jnp.int32, (HQ, KVH * DH), 0)
    col = lax.broadcasted_iota(jnp.int32, (HQ, KVH * DH), 1)
    bd[...] = jnp.where(row // groups == col // DH, 1.0, 0.0).astype(jnp.bfloat16)
    pn[pages_dev] = jnp.zeros((HQ, DH), jnp.float32)
    pt[pages_dev] = jnp.zeros((HQ, DH), jnp.float32)
    pm[pages_dev] = jnp.full((HQ, DH), LOW, jnp.float32)
    pl.semaphore_wait(barrier, n - 1)

    def q_copy(src, dst, sem):
        return pltpu.make_async_remote_copy(
            src_ref=qg.at[src], dst_ref=qg.at[src], send_sem=sem, recv_sem=q_recv.at[src],
            device_id={"seq": dst},
        )

    @pl.loop(1, chips)
    def _(k):
        q_copy(me, lax.rem(me + 2 * k, n), q_send.at[k]).start()

    q_copy(me, sib, f_send.at[0]).start()

    @pl.loop(1, chips)
    def _(k):
        src = lax.rem(me + n - 2 * k, n)
        q_copy(src, sib, q_send.at[k]).wait_recv()
        q_copy(src, sib, f_send.at[k]).start()

    @pl.loop(0, chips)
    def _(k):
        q_copy(lax.rem(sib + n - 2 * k, n), sib, f_send.at[k]).wait_recv()

    lane = lax.broadcasted_iota(jnp.int32, (HQ, page_len), 1)

    @pl.loop(0, pages_dev, unroll=4)
    def _(p):
        kv_copy(p).wait()
        q = qg[meta[p] // req_dev, lax.rem(meta[p], req_dev)]
        qb = jnp.concatenate([q] * KVH, axis=1) * bd[...]
        s = lax.dot_general(
            qb, kv[p, 0], (((1,), (1,)), ((), ())), preferred_element_type=jnp.float32
        ) * scale
        s = jnp.where(lane < meta[2 * pages_dev + p], s, LOW)
        m = jnp.max(s, axis=1, keepdims=True)
        e = jnp.exp(s - m)
        t = jnp.sum(e, axis=1, keepdims=True)
        full = jnp.dot(e.astype(jnp.bfloat16), kv[p, 1], preferred_element_type=jnp.float32)
        pn[p] = jnp.concatenate(
            [full[g * groups:(g + 1) * groups, g * DH:(g + 1) * DH] for g in range(KVH)], axis=0
        )
        pm[p] = jnp.broadcast_to(m, (HQ, DH))
        pt[p] = jnp.broadcast_to(t, (HQ, DH))

    @pl.loop(0, pages_dev)
    def _(p):
        b = meta[pages_dev + p]
        m0 = pm[b]
        m1 = pm[p]
        m = jnp.maximum(m0, m1)
        a0 = jnp.exp(m0 - m)
        a1 = jnp.exp(m1 - m)
        pn[p] = pn[b] * a0 + pn[p] * a1
        pt[p] = pt[b] * a0 + pt[p] * a1
        pm[p] = m

    wide = lax.broadcasted_iota(jnp.int32, (HQ, 128), 1)

    def ml_copy(d, k):
        return pltpu.make_async_remote_copy(
            src_ref=mls.at[d], dst_ref=mlr.at[me], send_sem=m_send.at[k], recv_sem=m_recv.at[me],
            device_id={"seq": d},
        )

    def ml_from(s):
        return pltpu.make_async_remote_copy(
            src_ref=mls.at[s], dst_ref=mlr.at[s], send_sem=m_send.at[0], recv_sem=m_recv.at[s],
            device_id={"seq": s},
        )

    def a_copy(d, k):
        return pltpu.make_async_remote_copy(
            src_ref=snd.at[d], dst_ref=rcv.at[me], send_sem=a_send.at[k], recv_sem=a_recv.at[me],
            device_id={"seq": d},
        )

    def a_from(s):
        return pltpu.make_async_remote_copy(
            src_ref=snd.at[s], dst_ref=rcv.at[s], send_sem=a_send.at[0], recv_sem=a_recv.at[s],
            device_id={"seq": s},
        )

    @pl.loop(0, blocks)
    def _(b):
        def put(c, carry):
            m, t = carry
            x = meta[3 * pages_dev + b * 128 + c]
            hit = wide == c
            return jnp.where(hit, pm[x], m), jnp.where(hit, pt[x], t)

        zero = jnp.zeros((HQ, 128), jnp.float32)
        m, t = lax.fori_loop(0, 128, put, (zero, zero), unroll=8)
        flip = jnp.concatenate([m, t, m, t], axis=0).T
        mls[pl.ds(b * per_block, per_block)] = flip.reshape(per_block, req_dev, 128)

    @pl.loop(1, n)
    def _(k):
        ml_copy(lax.rem(me + k, n), k).start()

    def fill(d):
        for i in range(req_dev):
            x = meta[3 * pages_dev + d * req_dev + i]
            t = pt[x]
            snd[d, i] = (pn[x] / jnp.where(t > 0, t, 1.0)).astype(jnp.bfloat16)

    @pl.loop(1, n)
    def _(k):
        d = lax.rem(me + k, n)
        fill(d)
        a_copy(d, k).start()

    fill(me)
    rcv[me] = snd[me]
    mlr[me] = mls[me]

    @pl.loop(1, n)
    def _(k):
        ml_from(lax.rem(me + n - k, n)).wait_recv()

    top = lax.fori_loop(0, n, lambda s, m: jnp.maximum(m, mlr[s]), mlr[0])

    def weigh(s, total):
        x = mlr[s]
        w = jnp.exp(x - top) * pltpu.roll(x, 128 - HQ, 1)
        wts[pl.ds(s * req_dev, req_dev), :] = w
        return total + w

    total = lax.fori_loop(0, n, weigh, jnp.zeros((req_dev, 128), jnp.float32))
    head = lax.broadcasted_iota(jnp.int32, (req_dev, 128), 1) < HQ
    inv = jnp.where(head, 1.0 / jnp.where(head, total, 1.0), 0.0)

    @pl.loop(0, n)
    def _(s):
        at = pl.ds(s * req_dev, req_dev)
        wts[at, :] = jnp.where(head, wts[at, :], 0.0) * inv

    @pl.loop(0, blocks)
    def _(b):
        wtt[b] = wts[pl.ds(b * 128, 128), :].T

    def add(s, first):
        w = wtt[s // per_block, 0:HQ, :]
        base = lax.rem(s, per_block) * req_dev
        for i in range(req_dev):
            c = jnp.sum(jnp.where(wide == base + i, w, 0.0), axis=1, keepdims=True)
            term = rcv[s, i].astype(jnp.float32) * c
            at = pl.ds(i * HQ, HQ)
            acc[at, :] = term if first else acc[at, :] + term

    add(me, True)

    @pl.loop(1, n)
    def _(k):
        s = lax.rem(me + n - k, n)
        a_from(s).wait_recv()
        add(s, False)

    for h in range(HQ):
        o_ref[:, h * DH:(h + 1) * DH] = acc[pl.ds(h, req_dev, stride=HQ), :].astype(jnp.bfloat16)

    @pl.loop(1, chips)
    def _(k):
        q_copy(me, sib, q_send.at[k]).wait_send()

    @pl.loop(0, chips)
    def _(k):
        q_copy(me, sib, f_send.at[k]).wait_send()

    @pl.loop(1, n)
    def _(k):
        d = lax.rem(me + k, n)
        ml_copy(d, k).wait_send()
        a_copy(d, k).wait_send()


def local(n, query, kv_pages, page_table, context_len):
    pages_dev = kv_pages.shape[0]
    page_len = kv_pages.shape[2]
    max_slots = page_table.shape[1]
    req_dev, width = query.shape
    reqs = page_table.shape[0]
    i32 = jnp.int32
    gp = lax.axis_index("seq") * pages_dev + jnp.arange(pages_dev, dtype=i32)
    none = reqs * max_slots
    spot = (
        jnp.arange(reqs, dtype=i32)[:, None] * max_slots + jnp.arange(max_slots, dtype=i32)[None, :]
    )
    code = jnp.min(
        jnp.where(page_table[None] == gp[:, None, None], spot[None], none), axis=(1, 2)
    )
    req = code // max_slots
    slot = code % max_slots
    ids = jnp.arange(pages_dev, dtype=i32)
    same = (req[:, None] == req[None, :]) & (ids[None, :] < ids[:, None]) & (code < none)[:, None]
    prev = jnp.max(jnp.where(same, ids[None, :], -1), axis=1)
    prev = jnp.where(prev < 0, pages_dev, prev)
    hot = req[:, None] == jnp.arange(reqs, dtype=i32)[None, :]
    length = jnp.sum(jnp.where(hot, context_len[None, :], 0), axis=1)
    vlen = jnp.where(code < none, jnp.clip(length - slot * page_len, 1, page_len), page_len)
    last = jnp.max(jnp.where(hot, ids[:, None], -1), axis=0)
    last = jnp.where(last < 0, pages_dev, last)
    meta = jnp.concatenate([jnp.where(code < none, req, 0), prev, vlen, last])
    f32, bf16 = jnp.float32, jnp.bfloat16
    dma = pltpu.SemaphoreType.DMA
    return pl.pallas_call(
        functools.partial(kernel, n, req_dev, pages_dev, page_len, DH ** (-0.5)),
        out_shape=jax.ShapeDtypeStruct((req_dev, width), bf16),
        in_specs=[
            pl.BlockSpec(memory_space=pltpu.SMEM),
            pl.BlockSpec(memory_space=pltpu.VMEM),
            pl.BlockSpec(memory_space=pl.ANY),
        ],
        out_specs=pl.BlockSpec(memory_space=pltpu.VMEM),
        scratch_shapes=[
            pltpu.VMEM(kv_pages.shape, bf16),
            pltpu.VMEM((n, req_dev, HQ, DH), bf16),
            pltpu.VMEM((req_dev * HQ, DH), f32),
            pltpu.VMEM((HQ, KVH * DH), bf16),
            pltpu.VMEM((pages_dev + 1, HQ, DH), f32),
            pltpu.VMEM((pages_dev + 1, HQ, DH), f32),
            pltpu.VMEM((pages_dev + 1, HQ, DH), f32),
            pltpu.VMEM((n, req_dev, HQ, DH), bf16),
            pltpu.VMEM((n, req_dev, HQ, DH), bf16),
            pltpu.VMEM((n, req_dev, 128), f32),
            pltpu.VMEM((n, req_dev, 128), f32),
            pltpu.VMEM((n * req_dev, 128), f32),
            pltpu.VMEM((n * req_dev // 128, 128, 128), f32),
            pltpu.VMEM((req_dev * HQ, DH), f32),
            dma((pages_dev,)),
            dma((n // 2,)),
            dma((n // 2,)),
            dma((n,)),
            dma((n,)),
            dma((n,)),
            dma((n,)),
            dma((n,)),
        ],
        compiler_params=pltpu.CompilerParams(
            collective_id=0, has_side_effects=True, vmem_limit_bytes=60 * 1024 * 1024
        ),
    )(meta, query, kv_pages)


def solution(mesh):
    placed = (
        P(("groups", "seq"), None),
        P(("groups", "seq"), None, None, None),
        P("groups", None),
        P("groups"),
    )
    return jax.shard_map(
        functools.partial(local, mesh.shape["seq"]),
        mesh=mesh, in_specs=placed, out_specs=P(("groups", "seq"), None), check_vma=False,
    )
```

```python
import functools

import jax
import jax.numpy as jnp
from jax import lax
from jax.experimental import pallas as pl
from jax.experimental.pallas import tpu as pltpu
from jax.sharding import PartitionSpec as P

HQ = 32
KVH = 4
DH = 128
LOW = -1e30


def kernel(
    n, req_dev, pages_dev, page_len, scale,
    table, ctx, q_ref, kv_ref, o_ref,
    kv, qg, qtmp, bd, pn, pm, pt, mv, meta, snd, rcx, mxs, mxr, cfs, out, rcv, mls, mlr, wts, wtt, acc,
    kv_sem, meta_sem, q_send, y_send, f_send, q_recv, x_send, x_recv, mx_send, mx_recv,
    a_send, a_recv, m_send, m_recv,
):
    me = lax.axis_index("seq")
    core = lax.rem(me, 2)
    chip = me // 2
    groups = HQ // KVH
    chips = n // 2
    rows = chips // 2
    zz = chip // 2
    yy = lax.rem(chip, 2)
    sib = chip * 2 + 1 - core
    per_block = 128 // req_dev
    blocks = n // per_block
    f32, i32, bf16 = jnp.float32, jnp.int32, jnp.bfloat16

    def dev(z, y):
        return (lax.rem(z + rows, rows) * 2 + y) * 2 + core

    ypeer = dev(zz, 1 - yy)

    def kv_copy(p):
        return pltpu.make_async_copy(kv_ref.at[p], kv.at[p], kv_sem.at[p])

    barrier = pltpu.get_barrier_semaphore()

    @pl.loop(1, n)
    def _(k):
        pl.semaphore_signal(barrier, inc=1, device_id={"seq": lax.rem(me + k, n)})

    @pl.loop(0, pages_dev)
    def _(p):
        kv_copy(p).start()

    for h in range(HQ):
        qtmp[pl.ds(h, req_dev, stride=HQ), :] = q_ref[:, h * DH:(h + 1) * DH].astype(f32)
    qg[me] = qtmp[...].astype(bf16).reshape(req_dev, HQ, DH)
    row = lax.broadcasted_iota(i32, (HQ, KVH * DH), 0)
    col = lax.broadcasted_iota(i32, (HQ, KVH * DH), 1)
    bd[...] = jnp.where(row // groups == col // DH, 1.0, 0.0).astype(bf16)
    pn[pages_dev] = jnp.zeros((HQ, DH), f32)
    pt[pages_dev] = jnp.zeros((HQ, DH), f32)
    pm[pages_dev] = jnp.full((HQ, DH), LOW, f32)
    wts[...] = jnp.zeros(wts.shape, f32)
    pl.semaphore_wait(barrier, n - 1)

    def q_copy(src, dst, sem):
        return pltpu.make_async_remote_copy(
            src_ref=qg.at[src], dst_ref=qg.at[src], send_sem=sem, recv_sem=q_recv.at[src],
            device_id={"seq": dst},
        )

    q_copy(me, ypeer, q_send.at[0]).start()

    @pl.loop(1, rows)
    def _(k):
        q_copy(me, dev(zz + k, yy), q_send.at[k]).start()

    q_copy(me, sib, f_send.at[0]).start()

    reqs, slots = table.shape
    none = reqs * slots
    lane1 = lax.broadcasted_iota(i32, (1, 128), 1)
    spot = lax.broadcasted_iota(i32, (reqs, slots), 0) * slots + lax.broadcasted_iota(
        i32, (reqs, slots), 1
    )

    def find(p, code):
        hit = jnp.where(table[...] == me * pages_dev + p, spot, none)
        best = jnp.min(jnp.min(hit, axis=0, keepdims=True), axis=1, keepdims=True)
        return jnp.where(lane1 == p, best, code)

    code = lax.fori_loop(0, pages_dev, find, jnp.full((1, 128), none, i32), unroll=4)
    req = code // slots
    sub = lax.broadcasted_iota(i32, (128, 128), 0)
    lanes = lax.broadcasted_iota(i32, (128, 128), 1)
    req_rows = jnp.broadcast_to(req, (128, 128))
    req_cols = req_rows.T
    live = code < none
    same = jnp.where((req_cols == req_rows) & (sub < lanes), sub, -1)
    prev = jnp.max(same, axis=0, keepdims=True)
    length = jnp.zeros((1, 128), i32)
    for b in range(reqs // 128):
        ctx_cols = jnp.broadcast_to(ctx[:, b * 128:(b + 1) * 128], (128, 128)).T
        length += jnp.sum(
            jnp.where(sub + b * 128 == req_rows, ctx_cols, 0), axis=0, keepdims=True
        )
        last = jnp.max(jnp.where(req_cols == lanes + b * 128, sub, -1), axis=0, keepdims=True)
        mv[3 + b:4 + b, :] = jnp.where(last < 0, pages_dev, last)
    mv[0:1, :] = jnp.where(live, req, 0)
    mv[1:2, :] = jnp.where(live & (prev >= 0), prev, pages_dev)
    left = jnp.minimum(jnp.maximum(length - (code - req * slots) * page_len, 1), page_len)
    mv[2:3, :] = jnp.where(live, left, page_len)
    meta_copy = pltpu.make_async_copy(mv, meta, meta_sem)
    meta_copy.start()

    @pl.loop(1, rows)
    def _(k):
        src = dev(zz - k, yy)
        q_copy(src, sib, f_send.at[k]).wait_recv()
        q_copy(src, ypeer, y_send.at[k]).start()
        q_copy(src, sib, f_send.at[k]).start()

    @pl.loop(0, rows)
    def _(k):
        src = dev(zz - k, 1 - yy)
        q_copy(src, sib, f_send.at[rows + k]).wait_recv()
        q_copy(src, sib, f_send.at[rows + k]).start()

    @pl.loop(0, pages_dev)
    def _(p):
        kv_copy(p).wait()

    meta_copy.wait()

    @pl.loop(0, chips)
    def _(k):
        q_copy(lax.rem(sib + n - 2 * k, n), sib, f_send.at[k]).wait_recv()

    lane = lax.broadcasted_iota(i32, (HQ, page_len), 1)
    batch = 8 if pages_dev % 8 == 0 else 1

    @pl.loop(0, pages_dev // batch)
    def _(c):
        ps = [c * batch + u for u in range(batch)]
        ss = []
        for p in ps:
            r = meta[0, p]
            q = qg[r // req_dev, lax.rem(r, req_dev)]
            qb = jnp.concatenate([q] * KVH, axis=1) * bd[...]
            s = lax.dot_general(
                qb, kv[p, 0], (((1,), (1,)), ((), ())), preferred_element_type=f32
            ) * scale
            ss.append(jnp.where(lane < meta[2, p], s, LOW))
        ms = [jnp.max(s, axis=1, keepdims=True) for s in ss]
        es = [jnp.exp(s - m) for s, m in zip(ss, ms)]
        ts = [jnp.sum(e, axis=1, keepdims=True) for e in es]
        ns = []
        for p, e in zip(ps, es):
            full = jnp.dot(e.astype(bf16), kv[p, 1], preferred_element_type=f32)
            ns.append(jnp.concatenate(
                [full[g * groups:(g + 1) * groups, g * DH:(g + 1) * DH] for g in range(KVH)],
                axis=0,
            ))
        for p, m, t, x in zip(ps, ms, ts, ns):
            pn[p] = x
            pm[p] = jnp.broadcast_to(m, (HQ, DH))
            pt[p] = jnp.broadcast_to(t, (HQ, DH))

    @pl.loop(0, pages_dev)
    def _(p):
        b = meta[1, p]
        m0 = pm[b]
        m1 = pm[p]
        m = jnp.maximum(m0, m1)
        a0 = jnp.exp(m0 - m)
        a1 = jnp.exp(m1 - m)
        pn[p] = pn[b] * a0 + pn[p] * a1
        pt[p] = pt[b] * a0 + pt[p] * a1
        pm[p] = m

    wide = lax.broadcasted_iota(i32, (HQ, 128), 1)

    def last_of(r):
        return meta[3 + r // 128, lax.rem(r, 128)]

    @pl.loop(0, blocks)
    def _(b):
        def put(c, carry):
            m, t = carry
            x = meta[3 + b, c]
            hit = wide == c
            return jnp.where(hit, pm[x], m), jnp.where(hit, pt[x], t)

        zero = jnp.zeros((HQ, 128), f32)
        m, t = lax.fori_loop(0, 128, put, (zero, zero), unroll=8)
        mxs[b, 0:HQ, :] = m
        mxs[b, HQ:2 * HQ, :] = t

    mx_copy = pltpu.make_async_remote_copy(
        src_ref=mxs, dst_ref=mxr, send_sem=mx_send, recv_sem=mx_recv, device_id={"seq": sib}
    )
    mx_copy.start()

    def x_copy(j):
        return pltpu.make_async_remote_copy(
            src_ref=snd.at[j], dst_ref=rcx.at[j], send_sem=x_send.at[j], recv_sem=x_recv.at[j],
            device_id={"seq": sib},
        )

    @pl.loop(1, chips + 1)
    def _(k):
        j = lax.rem(chip + k, chips)
        for i in range(req_dev):
            x = last_of((j * 2 + 1 - core) * req_dev + i)
            t = pt[x]
            snd[j, i] = (pn[x] / jnp.where(t > 0, t, 1.0)).astype(bf16)
        x_copy(j).start()

    mx_copy.wait_recv()

    @pl.loop(0, blocks)
    def _(b):
        m0, t0 = mxs[b, 0:HQ, :], mxs[b, HQ:2 * HQ, :]
        m1, t1 = mxr[b, 0:HQ, :], mxr[b, HQ:2 * HQ, :]
        m = jnp.maximum(m0, m1)
        e0 = jnp.exp(m0 - m)
        e1 = jnp.exp(m1 - m) * t1
        t = e0 * t0 + e1
        inv = 1.0 / jnp.where(t > 0, t, 1.0)
        cfs[b, 0:HQ, :] = e0 * inv
        cfs[b, HQ:2 * HQ, :] = e1 * inv
        flip = jnp.concatenate([m, t, m, t], axis=0).T
        mls[pl.ds(b * per_block, per_block)] = flip.reshape(per_block, req_dev, 128)

    def ml_copy(j):
        d = j * 2 + core
        return pltpu.make_async_remote_copy(
            src_ref=mls.at[d], dst_ref=mlr.at[chip], send_sem=m_send.at[j],
            recv_sem=m_recv.at[chip], device_id={"seq": d},
        )

    def ml_from(j):
        return pltpu.make_async_remote_copy(
            src_ref=mls.at[j], dst_ref=mlr.at[j], send_sem=m_send.at[j], recv_sem=m_recv.at[j],
            device_id={"seq": j * 2 + core},
        )

    def a_copy(j):
        return pltpu.make_async_remote_copy(
            src_ref=out.at[j], dst_ref=rcv.at[chip], send_sem=a_send.at[j],
            recv_sem=a_recv.at[chip], device_id={"seq": j * 2 + core},
        )

    def a_from(j):
        return pltpu.make_async_remote_copy(
            src_ref=out.at[j], dst_ref=rcv.at[j], send_sem=a_send.at[j], recv_sem=a_recv.at[j],
            device_id={"seq": j * 2 + core},
        )

    @pl.loop(1, chips)
    def _(k):
        ml_copy(lax.rem(chip + k, chips)).start()

    def merge(j, ref):
        x_copy(j).wait_recv()
        for i in range(req_dev):
            r = (j * 2 + core) * req_dev + i
            hit = jnp.concatenate([wide, wide], axis=0) == lax.rem(r, 128)
            c = jnp.sum(jnp.where(hit, cfs[r // 128], 0.0), axis=1, keepdims=True)
            mine = pn[last_of(r)] * c[0:HQ]
            ref[j, i] = (mine + rcx[j, i].astype(f32) * c[HQ:2 * HQ]).astype(bf16)

    @pl.loop(1, chips)
    def _(k):
        j = lax.rem(chip + k, chips)
        merge(j, out)
        a_copy(j).start()

    merge(chip, rcv)
    mlr[chip] = mls[me]

    @pl.loop(1, chips)
    def _(k):
        ml_from(lax.rem(chip + chips - k, chips)).wait_recv()

    top = lax.fori_loop(0, chips, lambda s, m: jnp.maximum(m, mlr[s]), mlr[0])

    def weigh(s, total):
        x = mlr[s]
        w = jnp.exp(x - top) * pltpu.roll(x, 128 - HQ, 1)
        wts[pl.ds(s * req_dev, req_dev), :] = w
        return total + w

    total = lax.fori_loop(0, chips, weigh, jnp.zeros((req_dev, 128), f32))
    head = lax.broadcasted_iota(i32, (req_dev, 128), 1) < HQ
    inv = jnp.where(head, 1.0 / jnp.where(head, total, 1.0), 0.0)

    @pl.loop(0, chips)
    def _(s):
        at = pl.ds(s * req_dev, req_dev)
        wts[at, :] = jnp.where(head, wts[at, :], 0.0) * inv

    @pl.loop(0, wts.shape[0] // 128)
    def _(b):
        wtt[b] = wts[pl.ds(b * 128, 128), :].T

    def add(s, first):
        w = wtt[s // per_block, 0:HQ, :]
        base = lax.rem(s, per_block) * req_dev
        for i in range(req_dev):
            c = jnp.sum(jnp.where(wide == base + i, w, 0.0), axis=1, keepdims=True)
            term = rcv[s, i].astype(f32) * c
            at = pl.ds(i * HQ, HQ)
            acc[at, :] = term if first else acc[at, :] + term

    add(chip, True)

    @pl.loop(1, chips)
    def _(k):
        s = lax.rem(chip + chips - k, chips)
        a_from(s).wait_recv()
        add(s, False)

    for h in range(HQ):
        o_ref[:, h * DH:(h + 1) * DH] = acc[pl.ds(h, req_dev, stride=HQ), :].astype(bf16)

    @pl.loop(0, rows)
    def _(k):
        q_copy(me, sib, q_send.at[k]).wait_send()

    @pl.loop(1, rows)
    def _(k):
        q_copy(me, sib, y_send.at[k]).wait_send()

    @pl.loop(0, chips)
    def _(k):
        q_copy(me, sib, f_send.at[k]).wait_send()
        x_copy(k).wait_send()

    mx_copy.wait_send()

    @pl.loop(1, chips)
    def _(k):
        j = lax.rem(chip + k, chips)
        ml_copy(j).wait_send()
        a_copy(j).wait_send()


def local(n, query, kv_pages, page_table, context_len):
    pages_dev, _, page_len, _ = kv_pages.shape
    req_dev, width = query.shape
    reqs = page_table.shape[0]
    blocks = reqs // 128
    chips = n // 2
    f32, bf16 = jnp.float32, jnp.bfloat16
    dma = pltpu.SemaphoreType.DMA
    vmem = pltpu.VMEM
    part = (chips, req_dev, HQ, DH)
    pages = (pages_dev + 1, HQ, DH)
    notes = ((3 + blocks + 7) // 8 * 8, 128)
    wide = (chips * req_dev + 127) // 128
    return pl.pallas_call(
        functools.partial(kernel, n, req_dev, pages_dev, page_len, DH ** (-0.5)),
        out_shape=jax.ShapeDtypeStruct((req_dev, width), bf16),
        in_specs=[
            pl.BlockSpec(memory_space=vmem),
            pl.BlockSpec(memory_space=vmem),
            pl.BlockSpec(memory_space=vmem),
            pl.BlockSpec(memory_space=pl.ANY),
        ],
        out_specs=pl.BlockSpec(memory_space=vmem),
        scratch_shapes=[
            vmem(kv_pages.shape, bf16),
            vmem((n, req_dev, HQ, DH), bf16),
            vmem((req_dev * HQ, DH), f32),
            vmem((HQ, KVH * DH), bf16),
            vmem(pages, f32),
            vmem(pages, f32),
            vmem(pages, f32),
            vmem(notes, jnp.int32),
            pltpu.SMEM(notes, jnp.int32),
            vmem(part, bf16),
            vmem(part, bf16),
            vmem((blocks, 2 * HQ, 128), f32),
            vmem((blocks, 2 * HQ, 128), f32),
            vmem((blocks, 2 * HQ, 128), f32),
            vmem(part, bf16),
            vmem(part, bf16),
            vmem((n, req_dev, 128), f32),
            vmem((chips, req_dev, 128), f32),
            vmem((wide * 128, 128), f32),
            vmem((wide, 128, 128), f32),
            vmem((req_dev * HQ, DH), f32),
            dma((pages_dev,)),
            dma,
            dma((chips // 2,)),
            dma((chips // 2,)),
            dma((chips,)),
            dma((n,)),
            dma((chips,)),
            dma((chips,)),
            dma,
            dma,
            dma((chips,)),
            dma((chips,)),
            dma((chips,)),
            dma((chips,)),
        ],
        compiler_params=pltpu.CompilerParams(
            collective_id=0, has_side_effects=True, vmem_limit_bytes=60 * 1024 * 1024
        ),
    )(page_table, context_len.reshape(1, reqs), query, kv_pages)


def solution(mesh):
    placed = (
        P(("groups", "seq"), None),
        P(("groups", "seq"), None, None, None),
        P("groups", None),
        P("groups"),
    )
    return jax.shard_map(
        functools.partial(local, mesh.shape["seq"]),
        mesh=mesh, in_specs=placed, out_specs=P(("groups", "seq"), None), check_vma=False,
    )
```

```python
import functools

import jax
import jax.numpy as jnp
from jax import lax
from jax.experimental import pallas as pl
from jax.experimental.pallas import tpu as pltpu
from jax.sharding import PartitionSpec as P

HQ = 32
KVH = 4
DH = 128
LOW = -1e30


def kernel(
    n, req_dev, pages_dev, page_len, scale,
    table, ctx, q_ref, kv_ref, o_ref,
    kv, qg, qtmp, bd, pn, pm, pt, mv, meta, snd, rcx, mxs, mxr, cfs, out, rcv, mls, mlr, wts, wtt, acc,
    kv_sem, meta_sem, q_send, y_send, f_send, q_recv, x_send, x_recv, mx_send, mx_recv,
    a_send, a_recv, m_send, m_recv,
):
    me = lax.axis_index("seq")
    core = lax.rem(me, 2)
    chip = me // 2
    groups = HQ // KVH
    chips = n // 2
    rows = chips // 2
    zz = chip // 2
    yy = lax.rem(chip, 2)
    sib = chip * 2 + 1 - core
    per_block = 128 // req_dev
    blocks = n // per_block
    f32, i32, bf16 = jnp.float32, jnp.int32, jnp.bfloat16

    def dev(z, y):
        return (lax.rem(z + rows, rows) * 2 + y) * 2 + core

    ypeer = dev(zz, 1 - yy)

    def kv_copy(p):
        return pltpu.make_async_copy(kv_ref.at[p], kv.at[p], kv_sem.at[p])

    barrier = pltpu.get_barrier_semaphore()

    pl.semaphore_signal(barrier, inc=1, device_id={"seq": sib})

    @pl.loop(1, chips)
    def _(k):
        pl.semaphore_signal(barrier, inc=1, device_id={"seq": lax.rem(me + 2 * k, n)})

    @pl.loop(0, pages_dev)
    def _(p):
        kv_copy(p).start()

    for h in range(HQ):
        qtmp[pl.ds(h, req_dev, stride=HQ), :] = q_ref[:, h * DH:(h + 1) * DH].astype(f32)
    qg[me] = qtmp[...].astype(bf16).reshape(req_dev, HQ, DH)
    row = lax.broadcasted_iota(i32, (HQ, KVH * DH), 0)
    col = lax.broadcasted_iota(i32, (HQ, KVH * DH), 1)
    bd[...] = jnp.where(row // groups == col // DH, 1.0, 0.0).astype(bf16)
    pn[pages_dev] = jnp.zeros((HQ, DH), f32)
    pt[pages_dev] = jnp.zeros((HQ, DH), f32)
    pm[pages_dev] = jnp.full((HQ, DH), LOW, f32)
    wts[...] = jnp.zeros(wts.shape, f32)
    pl.semaphore_wait(barrier, chips)

    def q_copy(src, dst, sem):
        return pltpu.make_async_remote_copy(
            src_ref=qg.at[src], dst_ref=qg.at[src], send_sem=sem, recv_sem=q_recv.at[src],
            device_id={"seq": dst},
        )

    q_copy(me, ypeer, q_send.at[0]).start()

    @pl.loop(1, rows)
    def _(k):
        q_copy(me, dev(zz + k, yy), q_send.at[k]).start()

    q_copy(me, sib, f_send.at[0]).start()

    reqs, slots = table.shape
    none = reqs * slots
    lane1 = lax.broadcasted_iota(i32, (1, 128), 1)
    spot = lax.broadcasted_iota(i32, (reqs, slots), 0) * slots + lax.broadcasted_iota(
        i32, (reqs, slots), 1
    )

    def find(p, code):
        hit = jnp.where(table[...] == me * pages_dev + p, spot, none)
        best = jnp.min(jnp.min(hit, axis=0, keepdims=True), axis=1, keepdims=True)
        return jnp.where(lane1 == p, best, code)

    code = lax.fori_loop(0, pages_dev, find, jnp.full((1, 128), none, i32), unroll=4)
    req = code // slots
    sub = lax.broadcasted_iota(i32, (128, 128), 0)
    lanes = lax.broadcasted_iota(i32, (128, 128), 1)
    req_rows = jnp.broadcast_to(req, (128, 128))
    req_cols = req_rows.T
    live = code < none
    same = jnp.where((req_cols == req_rows) & (sub < lanes), sub, -1)
    prev = jnp.max(same, axis=0, keepdims=True)
    length = jnp.zeros((1, 128), i32)
    for b in range(reqs // 128):
        ctx_cols = jnp.broadcast_to(ctx[:, b * 128:(b + 1) * 128], (128, 128)).T
        length += jnp.sum(
            jnp.where(sub + b * 128 == req_rows, ctx_cols, 0), axis=0, keepdims=True
        )
        last = jnp.max(jnp.where(req_cols == lanes + b * 128, sub, -1), axis=0, keepdims=True)
        mv[3 + b:4 + b, :] = jnp.where(last < 0, pages_dev, last)
    mv[0:1, :] = jnp.where(live, req, 0)
    mv[1:2, :] = jnp.where(live & (prev >= 0), prev, pages_dev)
    left = jnp.minimum(jnp.maximum(length - (code - req * slots) * page_len, 1), page_len)
    mv[2:3, :] = jnp.where(live, left, page_len)
    meta_copy = pltpu.make_async_copy(mv, meta, meta_sem)
    meta_copy.start()

    @pl.loop(1, rows)
    def _(k):
        src = dev(zz - k, yy)
        q_copy(src, sib, f_send.at[k]).wait_recv()
        q_copy(src, ypeer, y_send.at[k]).start()
        q_copy(src, sib, f_send.at[k]).start()

    @pl.loop(0, rows)
    def _(k):
        src = dev(zz - k, 1 - yy)
        q_copy(src, sib, f_send.at[rows + k]).wait_recv()
        q_copy(src, sib, f_send.at[rows + k]).start()

    @pl.loop(0, pages_dev)
    def _(p):
        kv_copy(p).wait()

    meta_copy.wait()

    @pl.loop(0, chips)
    def _(k):
        q_copy(lax.rem(sib + n - 2 * k, n), sib, f_send.at[k]).wait_recv()

    lane = lax.broadcasted_iota(i32, (HQ, page_len), 1)
    batch = max(u for u in (20, 8, 4, 1) if pages_dev % u == 0)

    @pl.loop(0, pages_dev // batch)
    def _(c):
        ps = [c * batch + u for u in range(batch)]
        ss = []
        for p in ps:
            r = meta[0, p]
            q = qg[r // req_dev, lax.rem(r, req_dev)]
            qb = jnp.concatenate([q] * KVH, axis=1) * bd[...]
            s = lax.dot_general(
                qb, kv[p, 0], (((1,), (1,)), ((), ())), preferred_element_type=f32
            ) * scale
            ss.append(jnp.where(lane < meta[2, p], s, LOW))
        ms = [jnp.max(s, axis=1, keepdims=True) for s in ss]
        es = [jnp.exp(s - m) for s, m in zip(ss, ms)]
        ts = [jnp.sum(e, axis=1, keepdims=True) for e in es]
        ns = []
        for p, e in zip(ps, es):
            full = jnp.dot(e.astype(bf16), kv[p, 1], preferred_element_type=f32)
            ns.append(jnp.concatenate(
                [full[g * groups:(g + 1) * groups, g * DH:(g + 1) * DH] for g in range(KVH)],
                axis=0,
            ))
        for p, m, t, x in zip(ps, ms, ts, ns):
            pn[p] = x
            pm[p] = jnp.broadcast_to(m, (HQ, DH))
            pt[p] = jnp.broadcast_to(t, (HQ, DH))

    @pl.loop(0, pages_dev)
    def _(p):
        b = meta[1, p]
        m0 = pm[b]
        m1 = pm[p]
        m = jnp.maximum(m0, m1)
        a0 = jnp.exp(m0 - m)
        a1 = jnp.exp(m1 - m)
        pn[p] = pn[b] * a0 + pn[p] * a1
        pt[p] = pt[b] * a0 + pt[p] * a1
        pm[p] = m

    wide = lax.broadcasted_iota(i32, (HQ, 128), 1)

    def last_of(r):
        return meta[3 + r // 128, lax.rem(r, 128)]

    @pl.loop(0, blocks)
    def _(b):
        def put(c, carry):
            m, t = carry
            x = meta[3 + b, c]
            hit = wide == c
            return jnp.where(hit, pm[x], m), jnp.where(hit, pt[x], t)

        zero = jnp.zeros((HQ, 128), f32)
        m, t = lax.fori_loop(0, 128, put, (zero, zero), unroll=8)
        mxs[b, 0:HQ, :] = m
        mxs[b, HQ:2 * HQ, :] = t

    mx_copy = pltpu.make_async_remote_copy(
        src_ref=mxs, dst_ref=mxr, send_sem=mx_send, recv_sem=mx_recv, device_id={"seq": sib}
    )
    mx_copy.start()

    def x_copy(j):
        return pltpu.make_async_remote_copy(
            src_ref=snd.at[j], dst_ref=rcx.at[j], send_sem=x_send.at[j], recv_sem=x_recv.at[j],
            device_id={"seq": sib},
        )

    @pl.loop(1, chips + 1)
    def _(k):
        j = lax.rem(chip + k, chips)
        for i in range(req_dev):
            x = last_of((j * 2 + 1 - core) * req_dev + i)
            t = pt[x]
            snd[j, i] = (pn[x] / jnp.where(t > 0, t, 1.0)).astype(bf16)
        x_copy(j).start()

    mx_copy.wait_recv()

    @pl.loop(0, blocks)
    def _(b):
        m0, t0 = mxs[b, 0:HQ, :], mxs[b, HQ:2 * HQ, :]
        m1, t1 = mxr[b, 0:HQ, :], mxr[b, HQ:2 * HQ, :]
        m = jnp.maximum(m0, m1)
        e0 = jnp.exp(m0 - m)
        e1 = jnp.exp(m1 - m) * t1
        t = e0 * t0 + e1
        inv = 1.0 / jnp.where(t > 0, t, 1.0)
        cfs[b, 0:HQ, :] = e0 * inv
        cfs[b, HQ:2 * HQ, :] = e1 * inv
        flip = jnp.concatenate([m, t, m, t], axis=0).T
        mls[pl.ds(b * per_block, per_block)] = flip.reshape(per_block, req_dev, 128)

    def ml_copy(j):
        d = j * 2 + core
        return pltpu.make_async_remote_copy(
            src_ref=mls.at[d], dst_ref=mlr.at[chip], send_sem=m_send.at[j],
            recv_sem=m_recv.at[chip], device_id={"seq": d},
        )

    def ml_from(j):
        return pltpu.make_async_remote_copy(
            src_ref=mls.at[j], dst_ref=mlr.at[j], send_sem=m_send.at[j], recv_sem=m_recv.at[j],
            device_id={"seq": j * 2 + core},
        )

    def a_copy(j):
        return pltpu.make_async_remote_copy(
            src_ref=out.at[j], dst_ref=rcv.at[chip], send_sem=a_send.at[j],
            recv_sem=a_recv.at[chip], device_id={"seq": j * 2 + core},
        )

    def a_from(j):
        return pltpu.make_async_remote_copy(
            src_ref=out.at[j], dst_ref=rcv.at[j], send_sem=a_send.at[j], recv_sem=a_recv.at[j],
            device_id={"seq": j * 2 + core},
        )

    @pl.loop(1, chips)
    def _(k):
        ml_copy(lax.rem(chip + k, chips)).start()

    def merge(j, ref):
        x_copy(j).wait_recv()
        for i in range(req_dev):
            r = (j * 2 + core) * req_dev + i
            hit = jnp.concatenate([wide, wide], axis=0) == lax.rem(r, 128)
            c = jnp.sum(jnp.where(hit, cfs[r // 128], 0.0), axis=1, keepdims=True)
            mine = pn[last_of(r)] * c[0:HQ]
            ref[j, i] = (mine + rcx[j, i].astype(f32) * c[HQ:2 * HQ]).astype(bf16)

    @pl.loop(1, chips)
    def _(k):
        j = lax.rem(chip + k, chips)
        merge(j, out)
        a_copy(j).start()

    merge(chip, rcv)
    mlr[chip] = mls[me]

    @pl.loop(1, chips)
    def _(k):
        ml_from(lax.rem(chip + chips - k, chips)).wait_recv()

    top = lax.fori_loop(0, chips, lambda s, m: jnp.maximum(m, mlr[s]), mlr[0])

    def weigh(s, total):
        x = mlr[s]
        w = jnp.exp(x - top) * pltpu.roll(x, 128 - HQ, 1)
        wts[pl.ds(s * req_dev, req_dev), :] = w
        return total + w

    total = lax.fori_loop(0, chips, weigh, jnp.zeros((req_dev, 128), f32))
    head = lax.broadcasted_iota(i32, (req_dev, 128), 1) < HQ
    inv = jnp.where(head, 1.0 / jnp.where(head, total, 1.0), 0.0)

    @pl.loop(0, chips)
    def _(s):
        at = pl.ds(s * req_dev, req_dev)
        wts[at, :] = jnp.where(head, wts[at, :], 0.0) * inv

    @pl.loop(0, wts.shape[0] // 128)
    def _(b):
        wtt[b] = wts[pl.ds(b * 128, 128), :].T

    def add(s, first):
        w = wtt[s // per_block, 0:HQ, :]
        base = lax.rem(s, per_block) * req_dev
        for i in range(req_dev):
            c = jnp.sum(jnp.where(wide == base + i, w, 0.0), axis=1, keepdims=True)
            term = rcv[s, i].astype(f32) * c
            at = pl.ds(i * HQ, HQ)
            acc[at, :] = term if first else acc[at, :] + term

    add(chip, True)

    @pl.loop(1, chips)
    def _(k):
        s = lax.rem(chip + chips - k, chips)
        a_from(s).wait_recv()
        add(s, False)

    for h in range(HQ):
        o_ref[:, h * DH:(h + 1) * DH] = acc[pl.ds(h, req_dev, stride=HQ), :].astype(bf16)

    @pl.loop(0, rows)
    def _(k):
        q_copy(me, sib, q_send.at[k]).wait_send()

    @pl.loop(1, rows)
    def _(k):
        q_copy(me, sib, y_send.at[k]).wait_send()

    @pl.loop(0, chips)
    def _(k):
        q_copy(me, sib, f_send.at[k]).wait_send()
        x_copy(k).wait_send()

    mx_copy.wait_send()

    @pl.loop(1, chips)
    def _(k):
        j = lax.rem(chip + k, chips)
        ml_copy(j).wait_send()
        a_copy(j).wait_send()


def local(n, query, kv_pages, page_table, context_len):
    pages_dev, _, page_len, _ = kv_pages.shape
    req_dev, width = query.shape
    reqs = page_table.shape[0]
    blocks = reqs // 128
    chips = n // 2
    f32, bf16 = jnp.float32, jnp.bfloat16
    dma = pltpu.SemaphoreType.DMA
    vmem = pltpu.VMEM
    part = (chips, req_dev, HQ, DH)
    pages = (pages_dev + 1, HQ, DH)
    notes = ((3 + blocks + 7) // 8 * 8, 128)
    wide = (chips * req_dev + 127) // 128
    return pl.pallas_call(
        functools.partial(kernel, n, req_dev, pages_dev, page_len, DH ** (-0.5)),
        out_shape=jax.ShapeDtypeStruct((req_dev, width), bf16),
        in_specs=[
            pl.BlockSpec(memory_space=vmem),
            pl.BlockSpec(memory_space=vmem),
            pl.BlockSpec(memory_space=vmem),
            pl.BlockSpec(memory_space=pl.ANY),
        ],
        out_specs=pl.BlockSpec(memory_space=vmem),
        scratch_shapes=[
            vmem(kv_pages.shape, bf16),
            vmem((n, req_dev, HQ, DH), bf16),
            vmem((req_dev * HQ, DH), f32),
            vmem((HQ, KVH * DH), bf16),
            vmem(pages, f32),
            vmem(pages, f32),
            vmem(pages, f32),
            vmem(notes, jnp.int32),
            pltpu.SMEM(notes, jnp.int32),
            vmem(part, bf16),
            vmem(part, bf16),
            vmem((blocks, 2 * HQ, 128), f32),
            vmem((blocks, 2 * HQ, 128), f32),
            vmem((blocks, 2 * HQ, 128), f32),
            vmem(part, bf16),
            vmem(part, bf16),
            vmem((n, req_dev, 128), f32),
            vmem((chips, req_dev, 128), f32),
            vmem((wide * 128, 128), f32),
            vmem((wide, 128, 128), f32),
            vmem((req_dev * HQ, DH), f32),
            dma((pages_dev,)),
            dma,
            dma((chips // 2,)),
            dma((chips // 2,)),
            dma((chips,)),
            dma((n,)),
            dma((chips,)),
            dma((chips,)),
            dma,
            dma,
            dma((chips,)),
            dma((chips,)),
            dma((chips,)),
            dma((chips,)),
        ],
        compiler_params=pltpu.CompilerParams(
            collective_id=0, has_side_effects=True, vmem_limit_bytes=60 * 1024 * 1024
        ),
    )(page_table, context_len.reshape(1, reqs), query, kv_pages)


def solution(mesh):
    placed = (
        P(("groups", "seq"), None),
        P(("groups", "seq"), None, None, None),
        P("groups", None),
        P("groups"),
    )
    return jax.shard_map(
        functools.partial(local, mesh.shape["seq"]),
        mesh=mesh, in_specs=placed, out_specs=P(("groups", "seq"), None), check_vma=False,
    )
```
